32 devices in a mesh: tm: 4 (over y, x), space: 8 (over z, core).
Axes of the slice: x: 2, y: 2, z: 4, core: 2. Of those that a mesh axis runs over, the one named last changes fastest.
Arguments:
- thermal_field: float32 [128, 49152], P(('tm', 'space')), may hold values from 245 to 255
- seasonal_bucket: int32 [128], replicated, may hold values from 0 to 45, as said below
- season_of_record: int32 [128], replicated, may hold values from 0 to 7
Outputs:
- anomaly: float32 [128, 49152], P(('tm', 'space'))
The draws below stay inside these ranges and needn't reach their ends.
Inputs may be any that keep to these rules, and one draw needn't show every extreme that they name: `seasonal_bucket`: every group holds at least one day whose year is below 6.
All inputs are finite; a program needn't handle non-finite values.
Results may differ from the reference program's by a relative error of at most 0.0003.
Values sent between devices are 32-bit elements; how exact they have to be, the bound alone decides.
No kernel may reach another device: no remote copies, remote signals or barrier semaphores. Data moves between devices by JAX's collectives and lax.ppermute only.
A program may use at most 64 MiB of HBM per device.

```python
import jax
import jax.numpy as jnp
from jax import lax

GROUPS = 46
YEARS = 8
BASE_YEARS = 6
TIME_STEPS = 128
MESH_POINTS = 49152


def calendar(key):
    ordering = jax.random.permutation(jax.random.fold_in(key, 11), TIME_STEPS)
    chosen_records = ordering[:GROUPS]
    random_group = jax.random.randint(jax.random.fold_in(key, 12), (TIME_STEPS,), 0, GROUPS)
    random_year = jax.random.randint(jax.random.fold_in(key, 13), (TIME_STEPS,), 0, YEARS)
    base_year = jax.random.randint(jax.random.fold_in(key, 14), (GROUPS,), 0, BASE_YEARS)
    groups = random_group.at[chosen_records].set(jnp.arange(GROUPS, dtype=jnp.int32))
    years = random_year.at[chosen_records].set(base_year)
    return (groups.astype(jnp.int32), years.astype(jnp.int32))


def draw_seasonal_bucket(key, part):
    return calendar(key)[0]


def draw_season_of_record(key, part):
    return calendar(key)[1]


def steps_of(rng, shape, pieces, least, high):
    def one(dim, blocks):
        steps = jax.random.uniform(jax.random.fold_in(jax.random.fold_in(rng, 6), dim), (blocks,), jnp.float32, least / len(pieces), high / len(pieces))
        return jnp.repeat(jnp.exp(steps), shape[dim] // blocks).reshape((-1,) + (1,) * (len(shape) - dim - 1))

    level = one(*pieces[0])
    for cut in pieces[1:]:
        level = level * one(*cut)
    return level


def setup_inputs(seed: int = 0) -> dict:
    splits = jax.random.split(jax.random.key(seed), 4)
    return {
        "thermal_field": jnp.clip(245.0 + 10.0 * jax.random.uniform(splits[0], (TIME_STEPS, MESH_POINTS), jnp.float32) ** steps_of(splits[0], (TIME_STEPS, MESH_POINTS), ((0, 32),), -0.2, 0.2), 245.0, 255.0),
        "seasonal_bucket": draw_seasonal_bucket(jax.random.fold_in(splits[3], 71), 0),
        "season_of_record": draw_season_of_record(jax.random.fold_in(splits[3], 71), 0),
    }


def reference(thermal_field, seasonal_bucket, season_of_record):
    group_ids = jnp.arange(GROUPS, dtype=jnp.int32)
    member = (seasonal_bucket[None, :] == group_ids[:, None]).astype(jnp.float32)
    reference_seasons = member * (season_of_record < BASE_YEARS).astype(jnp.float32)[None, :]
    counts = jnp.sum(reference_seasons, axis=1)
    bucket_aggregates = jnp.dot(reference_seasons, thermal_field, precision=lax.Precision.HIGHEST, preferred_element_type=jnp.float32)
    climate = bucket_aggregates / counts[:, None]
    chosen_records = jnp.dot(member.T, climate, precision=lax.Precision.HIGHEST, preferred_element_type=jnp.float32)
    return thermal_field - chosen_records
```

```python
import jax
import jax.numpy as jnp
from jax import lax
from jax.experimental import pallas as pl
from jax.experimental.pallas import tpu as pltpu
from jax.sharding import PartitionSpec as P

BASE_YEARS = 6
AXES = ("tm", "space")
VMEM = pl.BlockSpec(memory_space=pltpu.VMEM)
GRANT = pltpu.CompilerParams(vmem_limit_bytes=32 * 2**20)
SUBLANES = 8


def mates(bucket_ref, season_ref, same_ref, inverse_ref):
    days = bucket_ref.shape[1]
    across = jnp.broadcast_to(bucket_ref[...].astype(jnp.float32), (days, days))
    base = jnp.broadcast_to(season_ref[...], (days, days)) < BASE_YEARS
    same = jnp.where((across.T == across) & base, 1.0, 0.0)
    same_ref[...] = same.astype(jnp.bfloat16)
    counts = jnp.sum(same, axis=1, keepdims=True)
    inverse_ref[...] = jnp.broadcast_to(1.0 / counts, inverse_ref.shape)


def subtract_climate(same_ref, inverse_ref, field_ref, out_ref):
    devices, rows, width = field_ref.shape
    step = max(1, SUBLANES // rows)
    field = jnp.concatenate(
        [
            jnp.concatenate([field_ref[k + j] for j in range(step)], axis=0)
            for k in range(0, devices, step)
        ],
        axis=0,
    )
    high = field.astype(jnp.bfloat16)
    rest = field - high.astype(jnp.float32)
    middle = rest.astype(jnp.bfloat16)
    low = (rest - middle.astype(jnp.float32)).astype(jnp.bfloat16)
    same = same_ref[...]
    sums = jnp.dot(
        jnp.concatenate([same, same, same], axis=1),
        jnp.concatenate([high, middle, low], axis=0),
        preferred_element_type=jnp.float32,
    )
    anomaly = field - sums * inverse_ref[:, :1]
    for k in range(devices):
        out_ref[k] = anomaly[k * rows : (k + 1) * rows]


def shards(thermal_field, seasonal_bucket, season_of_record):
    days = seasonal_bucket.shape[0]
    rows, cells = thermal_field.shape
    devices = days // rows
    width = cells // devices
    same, inverse = pl.pallas_call(
        mates,
        in_specs=[VMEM, VMEM],
        out_specs=(VMEM, VMEM),
        compiler_params=GRANT,
        out_shape=(
            pltpu.VMEM((days, days), jnp.bfloat16),
            pltpu.VMEM((days, 128), jnp.float32),
        ),
    )(seasonal_bucket[None, :], season_of_record[None, :])
    blocks = lax.all_to_all(
        thermal_field.reshape(rows, devices, width), AXES, split_axis=1, concat_axis=0
    )
    anomaly = pl.pallas_call(
        subtract_climate,
        in_specs=[VMEM, VMEM, VMEM],
        out_specs=VMEM,
        compiler_params=GRANT,
        out_shape=pltpu.VMEM((devices, rows, width), jnp.float32),
    )(*(pltpu.with_memory_space_constraint(part, pltpu.VMEM) for part in (same, inverse, blocks)))
    result = lax.all_to_all(anomaly, AXES, split_axis=0, concat_axis=1)
    return result.reshape(rows, cells)


def solution(mesh):
    placed = (P(AXES, None), P(), P())
    return jax.shard_map(
        shards, mesh=mesh, in_specs=placed, out_specs=P(AXES, None), check_vma=False
    )
```

```python
import random

import jax
import jax.numpy as jnp
import numpy as np
from jax import lax
from jax.experimental import pallas as pl
from jax.experimental.pallas import tpu as pltpu
from jax.sharding import PartitionSpec as P

BASE_YEARS = 6
AXES = ("tm", "space")
VMEM = pl.BlockSpec(memory_space=pltpu.VMEM)
GRANT = pltpu.CompilerParams(vmem_limit_bytes=32 * 2**20)
SUBLANES = 8


def mates(bucket_ref, season_ref, same_ref, inverse_ref):
    days = bucket_ref.shape[1]
    across = jnp.broadcast_to(bucket_ref[...].astype(jnp.float32), (days, days))
    base = jnp.broadcast_to(season_ref[...], (days, days)) < BASE_YEARS
    same = jnp.where((across.T == across) & base, 1.0, 0.0)
    same_ref[...] = same.astype(jnp.bfloat16)
    counts = jnp.sum(same, axis=1, keepdims=True)
    inverse_ref[...] = jnp.broadcast_to(1.0 / counts, inverse_ref.shape)


def subtract_climate(same_ref, inverse_ref, field_ref, out_ref):
    devices, rows, width = field_ref.shape
    step = max(1, SUBLANES // rows)
    field = jnp.concatenate(
        [
            jnp.concatenate([field_ref[k + j] for j in range(step)], axis=0)
            for k in range(0, devices, step)
        ],
        axis=0,
    )
    high = field.astype(jnp.bfloat16)
    rest = field - high.astype(jnp.float32)
    middle = rest.astype(jnp.bfloat16)
    low = (rest - middle.astype(jnp.float32)).astype(jnp.bfloat16)
    same = same_ref[...]
    sums = jnp.dot(
        jnp.concatenate([same, same, same], axis=1),
        jnp.concatenate([high, middle, low], axis=0),
        preferred_element_type=jnp.float32,
    )
    anomaly = field - sums * inverse_ref[:, :1]
    for k in range(devices):
        out_ref[k] = anomaly[k * rows : (k + 1) * rows]


def ranks(devices):
    order = list(range(devices))
    random.Random(1).shuffle(order)
    return order


def shards(thermal_field, seasonal_bucket, season_of_record):
    days = seasonal_bucket.shape[0]
    rows, cells = thermal_field.shape
    devices = days // rows
    width = cells // devices
    order = ranks(devices)
    bucket, season = (
        jnp.take(days_of, np.asarray(order), axis=0).reshape(1, days)
        for days_of in (seasonal_bucket.reshape(devices, rows), season_of_record.reshape(devices, rows))
    )
    same, inverse = pl.pallas_call(
        mates,
        in_specs=[VMEM, VMEM],
        out_specs=(VMEM, VMEM),
        compiler_params=GRANT,
        out_shape=(
            pltpu.VMEM((days, days), jnp.bfloat16),
            pltpu.VMEM((days, 128), jnp.float32),
        ),
    )(bucket, season)
    blocks = lax.all_to_all(
        thermal_field.reshape(rows, devices, width), AXES, split_axis=1, concat_axis=0,
        axis_index_groups=[order],
    )
    anomaly = pl.pallas_call(
        subtract_climate,
        in_specs=[VMEM, VMEM, VMEM],
        out_specs=VMEM,
        compiler_params=GRANT,
        out_shape=pltpu.VMEM((devices, rows, width), jnp.float32),
    )(*(pltpu.with_memory_space_constraint(part, pltpu.VMEM) for part in (same, inverse, blocks)))
    result = lax.all_to_all(
        anomaly, AXES, split_axis=0, concat_axis=1, axis_index_groups=[order]
    )
    return result.reshape(rows, cells)


def solution(mesh):
    placed = (P(AXES, None), P(), P())
    return jax.shard_map(
        shards, mesh=mesh, in_specs=placed, out_specs=P(AXES, None), check_vma=False
    )
```
